256 devices in a mesh: site: 4 (over z_lo), py: 8 (over z_hi, x), px: 4 (over y), pz: 2 (over core).
Axes of the slice: x: 4, y: 4, z: 8 (z_hi: 2, z_lo: 4; z = z_hi * 4 + z_lo), core: 2. Of those that a mesh axis runs over, the one named last changes fastest.
Arguments:
- initial_heat_state: float32 [128, 256, 64, 128], P(('site', 'py'), 'px', 'pz'), parts along dimension 0, may hold values from 0.2 to 1.8
- scaled_speed_north: float32 [128, 256, 64, 128], P(('site', 'py'), 'px', 'pz'), parts along dimension 0, may hold values from -0.3 to 0.3
- scaled_speed_east: float32 [128, 256, 64, 128], P(('site', 'py'), 'px', 'pz'), parts along dimension 0, may hold values from -0.3 to 0.3
- scaled_speed_upward: float32 [128, 256, 64, 128], P(('site', 'py'), 'px', 'pz'), parts along dimension 0, may hold values from -0.3 to 0.3
Outputs:
- temperature_end: float32 [128, 256, 64, 128], P(('site', 'py'), 'px', 'pz'), parts along dimension 0
The draws below stay inside these ranges and needn't reach their ends.
There are 4 independent parts, one for each index of `site`. The reference program is written for one: setup_inputs(seed, part) draws one part's arguments, and reference() takes and returns one part's arrays. A program takes and returns all parts, laid end to end along the dimension named above; each array names one. Nothing has to cross between parts.
All inputs are finite; a program needn't handle non-finite values.
Results may differ from the reference program's by a relative error of at most 0.00002.
Values sent between devices are 32-bit elements; how exact they have to be, the bound alone decides.
A program may use at most 256 MiB of HBM per device.

```python
import jax
import jax.numpy as jnp
from jax import lax

MESH_POINTS_NORTH = 32
MESH_POINTS_EAST = 256
MESH_POINTS_UP = 64
TRACER_TOTAL = 128
STEPS = 4


def block_scale(key, shape, pieces, least, largest):
    gain, own = 1.0, jax.random.fold_in(key, 6)
    for position, blocks in pieces:
        heights = jnp.exp(jax.random.uniform(jax.random.fold_in(own, position), (blocks,), jnp.float32, least / len(pieces), largest / len(pieces)))
        gain = gain * jnp.repeat(heights, shape[position] // blocks).reshape([-1 if axis == position else 1 for axis in range(len(shape))])
    return gain


def setup_inputs(seed: int = 0, part: int = 0) -> dict:
    splits = jax.random.split(jax.random.key(seed), 5)
    part_keys = jax.random.split(jax.random.fold_in(splits[4], part), 5)
    return {
        "initial_heat_state": jnp.clip(0.2 + 1.5999999 * jax.random.uniform(part_keys[0], (MESH_POINTS_NORTH, MESH_POINTS_EAST, MESH_POINTS_UP, TRACER_TOTAL), jnp.float32) ** block_scale(part_keys[0], (MESH_POINTS_NORTH, MESH_POINTS_EAST, MESH_POINTS_UP, TRACER_TOTAL), ((0, 8), (1, 4), (2, 2)), -0.2, 0.2), 0.2, 1.8),
        "scaled_speed_north": jnp.clip(jax.random.uniform(part_keys[1], (MESH_POINTS_NORTH, MESH_POINTS_EAST, MESH_POINTS_UP, TRACER_TOTAL), jnp.float32, -0.3, 0.3) * block_scale(part_keys[1], (MESH_POINTS_NORTH, MESH_POINTS_EAST, MESH_POINTS_UP, TRACER_TOTAL), ((0, 8), (1, 4), (2, 2)), -0.4, 0.0), -0.3, 0.3),
        "scaled_speed_east": jnp.clip(jax.random.uniform(part_keys[2], (MESH_POINTS_NORTH, MESH_POINTS_EAST, MESH_POINTS_UP, TRACER_TOTAL), jnp.float32, -0.3, 0.3) * block_scale(part_keys[2], (MESH_POINTS_NORTH, MESH_POINTS_EAST, MESH_POINTS_UP, TRACER_TOTAL), ((0, 8), (1, 4), (2, 2)), -0.4, 0.0), -0.3, 0.3),
        "scaled_speed_upward": jnp.clip(jax.random.uniform(part_keys[3], (MESH_POINTS_NORTH, MESH_POINTS_EAST, MESH_POINTS_UP, TRACER_TOTAL), jnp.float32, -0.3, 0.3) * block_scale(part_keys[3], (MESH_POINTS_NORTH, MESH_POINTS_EAST, MESH_POINTS_UP, TRACER_TOTAL), ((0, 8), (1, 4), (2, 2)), -0.4, 0.0), -0.3, 0.3),
    }


def strip_edges(values, dims):
    for dim in dims:
        values = lax.slice_in_dim(values, 1, values.shape[dim] - 1, axis=dim)
    return values


def neighbour(values, dim, start, dims):
    others = [other for other in dims if other != dim]
    values = strip_edges(values, others)
    return lax.slice_in_dim(values, start, start + values.shape[dim] - 2, axis=dim)


def march_once(padded_with_frame, scaled_speed_north, scaled_speed_east, scaled_speed_upward):
    middle = strip_edges(padded_with_frame, (0, 1, 2))
    lower = [neighbour(padded_with_frame, dim, 0, (0, 1, 2)) for dim in (0, 1, 2)]
    upper = [neighbour(padded_with_frame, dim, 2, (0, 1, 2)) for dim in (0, 1, 2)]
    slopes = [above - below for above, below in zip(upper, lower)]
    smooth_rate = 0.05
    spread = lower[0] + upper[0] + lower[1] + upper[1] + lower[2] + upper[2] - 6.0 * middle
    return middle - scaled_speed_north * slopes[0] - scaled_speed_east * slopes[1] - scaled_speed_upward * slopes[2] + smooth_rate * spread


def reference(initial_heat_state, scaled_speed_north, scaled_speed_east, scaled_speed_upward):
    for step in range(STEPS):
        initial_heat_state = march_once(jnp.pad(initial_heat_state, ((1, 1), (1, 1), (1, 1), (0, 0)), mode="constant"), scaled_speed_north, scaled_speed_east, scaled_speed_upward)
    return initial_heat_state
```

```python
import functools

import jax
import jax.numpy as jnp
from jax import lax
from jax.experimental import pallas as pl
from jax.experimental.pallas import tpu as pltpu
from jax.sharding import PartitionSpec as P

MESH = pl.DeviceIdType.MESH
STEPS = 4
NY, NX, NZ, NS = 4, 64, 32, 128
K = 16
XC = NX // K
DIRECT = 2
ZP = 8


def kernel(u, vn, ve, vu, out, U, V, H, *sems):
    (u_sem, v_sem, out_sem, h_send, h_recv, x_send, x_recv, z_send, z_recv) = sems
    py, px, pz = lax.axis_index("py"), lax.axis_index("px"), lax.axis_index("pz")
    has_lo, has_hi = py > 0, py < 7
    x_lo, x_hi = px > 0, px < 3
    relayed = pz == 1
    edge = (py == 0) | (py == 7)
    middle = (py == 3) | (py == 4)

    def chunk(i):
        half = i // 2
        return half + (i % 2) * (K - 1 - 2 * half)

    def cols(k):
        return pl.ds(k * XC, XC)

    def inner(k):
        return pl.ds(1 + k * XC, XC)

    def load_u(k):
        return pltpu.make_async_copy(
            u.at[:, cols(k)], U.at[0, :, inner(k), pl.ds(ZP, NZ)], u_sem.at[k]
        )

    def load_v(f, k):
        return pltpu.make_async_copy(
            (vn, ve, vu)[f].at[:, cols(k)], V.at[f, :, cols(k)], v_sem.at[f, k]
        )

    def store(k):
        return pltpu.make_async_copy(
            U.at[STEPS, :, inner(k), pl.ds(ZP, NZ)], out.at[:, cols(k)], out_sem.at[k]
        )

    def y_source(first, t, side, k):
        plane = (0, NY - 1)[side]
        if first:
            return u.at[plane, cols(k)]
        return U.at[t, plane, inner(k), pl.ds(ZP, NZ)]

    def y_copy(first, t, side, k, target, slot):
        return pltpu.make_async_remote_copy(
            src_ref=y_source(first, t, side, k),
            dst_ref=H.at[t, slot, cols(k)],
            send_sem=h_send.at[t, side, k],
            recv_sem=h_recv.at[t, slot, k],
            device_id={"py": target},
            device_id_type=MESH,
        )

    def through(t, i):
        late = (t == STEPS - 1) & (i >= K - DIRECT)
        return relayed & jnp.logical_not(late)

    def y_route(t, i, side):
        if side == 0:
            return jnp.where((py == 4) & through(t, i), 7, jnp.maximum(py - 1, 0)), 1
        return jnp.where((py == 3) & through(t, i), 0, jnp.minimum(py + 1, 7)), 0

    def send_y(first, t, i, k):
        @pl.when(has_lo)
        def _():
            y_copy(first, t, 0, k, *y_route(t, i, 0)).start()

        @pl.when(has_hi)
        def _():
            y_copy(first, t, 1, k, *y_route(t, i, 1)).start()

    def relay_copy(t, k):
        slot = jnp.where(py == 0, 0, 1)
        return pltpu.make_async_remote_copy(
            src_ref=H.at[t, slot, cols(k)],
            dst_ref=H.at[t, slot, cols(k)],
            send_sem=h_send.at[t, slot, k],
            recv_sem=h_recv.at[t, slot, k],
            device_id={"py": jnp.where(py == 0, 4, 3)},
            device_id_type=MESH,
        )

    def y_landed(t, slot, k):
        return pltpu.make_async_remote_copy(
            src_ref=H.at[t, slot, cols(k)],
            dst_ref=H.at[t, slot, cols(k)],
            send_sem=h_send.at[t, slot, k],
            recv_sem=h_recv.at[t, slot, k],
            device_id={"py": jnp.where(py == 0, 1, 0)},
            device_id_type=MESH,
        )

    def x_copy(first, t, side):
        src, dst = ((0, NX + 1), (NX - 1, 0))[side]
        source = u.at[:, src] if first else U.at[t, :, 1 + src, pl.ds(ZP, NZ)]
        return pltpu.make_async_remote_copy(
            src_ref=source,
            dst_ref=U.at[t, :, dst, pl.ds(ZP, NZ)],
            send_sem=x_send.at[t, side],
            recv_sem=x_recv.at[t, 1 - side],
            device_id={"px": (jnp.maximum(px - 1, 0), jnp.minimum(px + 1, 3))[side]},
            device_id_type=MESH,
        )

    def z_copy(first, t, k):
        start = pl.multiple_of((1 - pz) * (NZ - ZP), ZP)
        if first:
            source = u.at[:, cols(k), pl.ds(start, ZP)]
        else:
            source = U.at[t, :, inner(k), pl.ds(pl.multiple_of(start + ZP, ZP), ZP)]
        land = pl.multiple_of(pz * (NZ + ZP), ZP)
        return pltpu.make_async_remote_copy(
            src_ref=source,
            dst_ref=U.at[t, :, inner(k), pl.ds(land, ZP)],
            send_sem=z_send.at[t, k],
            recv_sem=z_recv.at[t, k],
            device_id={"pz": 1 - pz},
            device_id_type=MESH,
        )

    for i in range(K):
        load_u(chunk(i)).start()
    for i in range(K):
        for f in range(3):
            load_v(f, chunk(i)).start()

    barrier = pltpu.get_barrier_semaphore()

    def greet(cond, **where):
        @pl.when(cond)
        def _():
            pl.semaphore_signal(barrier, inc=1, device_id=where, device_id_type=MESH)

    greet(has_lo, py=jnp.maximum(py - 1, 0))
    greet(has_hi, py=jnp.minimum(py + 1, 7))
    greet(x_lo, px=jnp.maximum(px - 1, 0))
    greet(x_hi, px=jnp.minimum(px + 1, 3))
    greet(pz >= 0, pz=1 - pz)
    extra = relayed & (edge | middle)
    greet(extra, py=jnp.where(edge, 3, 0))
    greet(extra, py=jnp.where(edge, 4, 7))
    one = lambda c: c.astype(jnp.int32)
    peers = one(has_lo) + one(has_hi) + one(x_lo) + one(x_hi) + 1 + 2 * one(extra)
    pl.semaphore_wait(barrier, peers)

    @pl.when(x_lo)
    def _():
        x_copy(True, 0, 0).start()

    @pl.when(x_hi)
    def _():
        x_copy(True, 0, 1).start()

    def first_sends(i, _):
        k = chunk(i)
        send_y(True, 0, i, k)
        z_copy(True, 0, k).start()
        return 0

    lax.fori_loop(0, K, first_sends, 0)

    zero_slab = pl.multiple_of(pz * (NZ + ZP), ZP)

    def clear_z(n, _):
        t, y = n // NY, n % NY
        U[t, y, :, pl.ds(zero_slab, ZP), :] = jnp.zeros((NX + 2, ZP, NS), jnp.float32)
        return 0

    lax.fori_loop(0, STEPS * NY, clear_z, 0)

    def clear_x(cond, column):
        @pl.when(cond)
        def _():
            for t in range(STEPS):
                U[t, :, column, pl.ds(ZP, NZ), :] = jnp.zeros((NY, NZ, NS), jnp.float32)

    clear_x(jnp.logical_not(x_lo), 0)
    clear_x(jnp.logical_not(x_hi), NX + 1)

    def compute(t, k):
        def column(n, _):
            x = k * XC + n
            mid = pl.ds(ZP, NZ)
            lo = jnp.where(has_lo, H[t, 0, x], 0.0)
            hi = jnp.where(has_hi, H[t, 1, x], 0.0)
            c = [U[t, y, x + 1, mid, :] for y in range(NY)]
            around = [lo] + c + [hi]
            for y in range(NY):
                below, above = around[y], around[y + 2]
                left, right = U[t, y, x, mid, :], U[t, y, x + 2, mid, :]
                down = U[t, y, x + 1, pl.ds(ZP - 1, NZ), :]
                up = U[t, y, x + 1, pl.ds(ZP + 1, NZ), :]
                total = ((below + above) + (left + right)) + (down + up)
                flow = (
                    V[0, y, x] * (above - below)
                    + V[1, y, x] * (right - left)
                    + V[2, y, x] * (up - down)
                )
                spread = total - 6.0 * c[y]
                U[t + 1, y, x + 1, mid, :] = (c[y] - flow) + 0.05 * spread
            return 0

        lax.fori_loop(0, XC, column, 0)

    def sends(j):
        t, i = j // K, j % K
        k = chunk(i)

        @pl.when(t + 1 < STEPS)
        def _():
            send_y(False, t + 1, i, k)
            z_copy(False, t + 1, k).start()

            @pl.when((i == 0) & x_lo)
            def _():
                x_copy(False, t + 1, 0).start()

            @pl.when((i == 1) & x_hi)
            def _():
                x_copy(False, t + 1, 1).start()

        @pl.when(t + 1 == STEPS)
        def _():
            store(k).start()

    def iteration(j, _):
        t, i = j // K, j % K
        k = chunk(i)

        @pl.when(edge & through(t, i))
        def _():
            slot = jnp.where(py == 0, 0, 1)
            y_landed(t, slot, k).wait_recv()
            relay_copy(t, k).start()

        @pl.when(t == 0)
        def _():
            @pl.when(i == 0)
            def _():
                load_u(chunk(0)).wait()
                load_u(chunk(1)).wait()

            @pl.when(i + 2 < K)
            def _():
                load_u(chunk(jnp.minimum(i + 2, K - 1))).wait()

            for f in range(3):
                load_v(f, k).wait()

        @pl.when((i == 0) & x_lo)
        def _():
            x_landed(t, 0).wait_recv()

        @pl.when((i == 1) & x_hi)
        def _():
            x_landed(t, 1).wait_recv()

        z_copy(False, t, k).wait_recv()

        @pl.when(has_lo)
        def _():
            y_landed(t, 0, k).wait_recv()

        @pl.when(has_hi)
        def _():
            y_landed(t, 1, k).wait_recv()

        compute(t, k)

        @pl.when(j > 0)
        def _():
            sends(jnp.maximum(j - 1, 0))

        return 0

    def x_landed(t, side):
        column = (0, NX + 1)[side]
        return pltpu.make_async_remote_copy(
            src_ref=U.at[t, :, column, pl.ds(ZP, NZ)],
            dst_ref=U.at[t, :, column, pl.ds(ZP, NZ)],
            send_sem=x_send.at[t, side],
            recv_sem=x_recv.at[t, side],
            device_id={"px": jnp.where(px == 0, 1, 0)},
            device_id_type=MESH,
        )

    lax.fori_loop(0, STEPS * K, iteration, 0)
    sends(STEPS * K - 1)

    def finish(j, _):
        t, i = j // K, j % K
        k = chunk(i)

        @pl.when(has_lo | (edge & through(t, i)))
        def _():
            y_landed(t, 0, k).wait_send()

        @pl.when(has_hi | (edge & through(t, i)))
        def _():
            y_landed(t, 1, k).wait_send()

        z_copy(False, t, k).wait_send()
        return 0

    lax.fori_loop(0, STEPS * K, finish, 0)
    for t in range(STEPS):
        for side, there in ((0, x_lo), (1, x_hi)):

            @pl.when(there)
            def _():
                x_landed(t, side).wait_send()

    def stored(k, _):
        store(k).wait()
        return 0

    lax.fori_loop(0, K, stored, 0)


def body(u, vn, ve, vu):
    DMA = pltpu.SemaphoreType.DMA
    return pl.pallas_call(
        kernel,
        out_shape=jax.ShapeDtypeStruct(u.shape, u.dtype),
        in_specs=[pl.BlockSpec(memory_space=pl.ANY)] * 4,
        out_specs=pl.BlockSpec(memory_space=pl.ANY),
        scratch_shapes=[
            pltpu.VMEM((STEPS + 1, NY, NX + 2, NZ + 2 * ZP, NS), jnp.float32),
            pltpu.VMEM((3, NY, NX, NZ, NS), jnp.float32),
            pltpu.VMEM((STEPS, 2, NX, NZ, NS), jnp.float32),
            DMA((K,)),
            DMA((3, K)),
            DMA((K,)),
            DMA((STEPS, 2, K)),
            DMA((STEPS, 2, K)),
            DMA((STEPS, 2)),
            DMA((STEPS, 2)),
            DMA((STEPS, K)),
            DMA((STEPS, K)),
        ],
        compiler_params=pltpu.CompilerParams(
            collective_id=0, has_side_effects=True, vmem_limit_bytes=62 * 2**20
        ),
        name="march",
    )(u, vn, ve, vu)


def solution(mesh):
    spec = P(("site", "py"), "px", "pz", None)
    return jax.shard_map(
        body, mesh=mesh, in_specs=(spec,) * 4, out_specs=spec, check_vma=False
    )
```

```python
import functools

import jax
import jax.numpy as jnp
from jax import lax
from jax.experimental import pallas as pl
from jax.experimental.pallas import tpu as pltpu
from jax.sharding import PartitionSpec as P

MESH = pl.DeviceIdType.MESH
STEPS = 4
NY, NX, NZ, NS = 4, 64, 32, 128
K = 8
XC = NX // K
AHEAD = 4
PRE = 2
DIRECT = 1
ZP = 8


def kernel(u, vn, ve, vu, out, U, V, H, *sems):
    (u_sem, v_sem, out_sem, h_send, h_recv, x_send, x_recv, z_send, z_recv) = sems
    py, px, pz = lax.axis_index("py"), lax.axis_index("px"), lax.axis_index("pz")
    has_lo, has_hi = py > 0, py < 7
    x_lo, x_hi = px > 0, px < 3
    relayed = pz == 1
    edge = (py == 0) | (py == 7)
    middle = (py == 3) | (py == 4)

    def chunk(i):
        half = i // 2
        return half + (i % 2) * (K - 1 - 2 * half)

    def cols(k):
        return pl.ds(k * XC, XC)

    def inner(k):
        return pl.ds(1 + k * XC, XC)

    def load_u(k):
        return pltpu.make_async_copy(
            u.at[:, cols(k)], U.at[0, :, inner(k), pl.ds(ZP, NZ)], u_sem.at[k]
        )

    def load_v(f, k):
        return pltpu.make_async_copy(
            (vn, ve, vu)[f].at[:, cols(k)], V.at[f, :, cols(k)], v_sem.at[f, k]
        )

    def y_source(first, t, side, k):
        plane = (0, NY - 1)[side]
        if first:
            return u.at[plane, cols(k)]
        return U.at[t, plane, inner(k), pl.ds(ZP, NZ)]

    def y_copy(first, t, side, k, target, slot):
        return pltpu.make_async_remote_copy(
            src_ref=y_source(first, t, side, k),
            dst_ref=H.at[t, slot, cols(k)],
            send_sem=h_send.at[t, side, k],
            recv_sem=h_recv.at[t, slot, k],
            device_id={"py": target},
            device_id_type=MESH,
        )

    def through(t, i):
        late = (t == STEPS - 1) & (i >= K - DIRECT)
        return relayed & jnp.logical_not(late)

    def y_route(t, i, side):
        if side == 0:
            return jnp.where((py == 4) & through(t, i), 7, jnp.maximum(py - 1, 0)), 1
        return jnp.where((py == 3) & through(t, i), 0, jnp.minimum(py + 1, 7)), 0

    def send_y(first, t, i, k):
        @pl.when(has_lo)
        def _():
            y_copy(first, t, 0, k, *y_route(t, i, 0)).start()

        @pl.when(has_hi)
        def _():
            y_copy(first, t, 1, k, *y_route(t, i, 1)).start()

    def relay_copy(t, k):
        slot = jnp.where(py == 0, 0, 1)
        return pltpu.make_async_remote_copy(
            src_ref=H.at[t, slot, cols(k)],
            dst_ref=H.at[t, slot, cols(k)],
            send_sem=h_send.at[t, slot, k],
            recv_sem=h_recv.at[t, slot, k],
            device_id={"py": jnp.where(py == 0, 4, 3)},
            device_id_type=MESH,
        )

    def y_landed(t, slot, k):
        return pltpu.make_async_remote_copy(
            src_ref=H.at[t, slot, cols(k)],
            dst_ref=H.at[t, slot, cols(k)],
            send_sem=h_send.at[t, slot, k],
            recv_sem=h_recv.at[t, slot, k],
            device_id={"py": jnp.where(py == 0, 1, 0)},
            device_id_type=MESH,
        )

    def x_copy(first, t, side):
        src, dst = ((0, NX + 1), (NX - 1, 0))[side]
        source = u.at[:, src] if first else U.at[t, :, 1 + src, pl.ds(ZP, NZ)]
        return pltpu.make_async_remote_copy(
            src_ref=source,
            dst_ref=U.at[t, :, dst, pl.ds(ZP, NZ)],
            send_sem=x_send.at[t, side],
            recv_sem=x_recv.at[t, 1 - side],
            device_id={"px": (jnp.maximum(px - 1, 0), jnp.minimum(px + 1, 3))[side]},
            device_id_type=MESH,
        )

    def z_copy(first, t, k):
        start = pl.multiple_of((1 - pz) * (NZ - ZP), ZP)
        if first:
            source = u.at[:, cols(k), pl.ds(start, ZP)]
        else:
            source = U.at[t, :, inner(k), pl.ds(pl.multiple_of(start + ZP, ZP), ZP)]
        land = pl.multiple_of(pz * (NZ + ZP), ZP)
        return pltpu.make_async_remote_copy(
            src_ref=source,
            dst_ref=U.at[t, :, inner(k), pl.ds(land, ZP)],
            send_sem=z_send.at[t, k],
            recv_sem=z_recv.at[t, k],
            device_id={"pz": 1 - pz},
            device_id_type=MESH,
        )

    barrier = pltpu.get_barrier_semaphore()

    def greet(cond, **where):
        @pl.when(cond)
        def _():
            pl.semaphore_signal(barrier, inc=1, device_id=where, device_id_type=MESH)

    greet(has_lo, py=jnp.maximum(py - 1, 0))
    greet(has_hi, py=jnp.minimum(py + 1, 7))
    greet(x_lo, px=jnp.maximum(px - 1, 0))
    greet(x_hi, px=jnp.minimum(px + 1, 3))
    greet(pz >= 0, pz=1 - pz)
    extra = relayed & (edge | middle)
    greet(extra, py=jnp.where(edge, 3, 0))
    greet(extra, py=jnp.where(edge, 4, 7))
    one = lambda c: c.astype(jnp.int32)
    peers = one(has_lo) + one(has_hi) + one(x_lo) + one(x_hi) + 1 + 2 * one(extra)
    pl.semaphore_wait(barrier, peers)

    @pl.when(x_lo)
    def _():
        x_copy(True, 0, 0).start()

    @pl.when(x_hi)
    def _():
        x_copy(True, 0, 1).start()

    def first_sends(i, _):
        k = chunk(i)
        send_y(True, 0, i, k)
        z_copy(True, 0, k).start()
        return 0

    lax.fori_loop(0, K, first_sends, 0)

    for i in range(min(PRE + 2, K)):
        load_u(chunk(i)).start()
    for i in range(min(PRE, K)):
        for f in range(3):
            load_v(f, chunk(i)).start()

    zero_slab = pl.multiple_of(pz * (NZ + ZP), ZP)

    def clear_z(n, _):
        t, y = n // NY, n % NY
        U[t, y, :, pl.ds(zero_slab, ZP), :] = jnp.zeros((NX + 2, ZP, NS), jnp.float32)
        return 0

    lax.fori_loop(0, STEPS * NY, clear_z, 0)

    def clear_x(cond, column):
        @pl.when(cond)
        def _():
            for t in range(STEPS):
                U[t, :, column, pl.ds(ZP, NZ), :] = jnp.zeros((NY, NZ, NS), jnp.float32)

    clear_x(jnp.logical_not(x_lo), 0)
    clear_x(jnp.logical_not(x_hi), NX + 1)

    def compute(t, k, planes):
        def column(n, _):
            x = k * XC + n
            mid = pl.ds(ZP, NZ)
            for y in planes:
                here = U[t, y, x + 1, mid, :]
                if y == 0:
                    below = jnp.where(has_lo, H[t, 0, x], 0.0)
                else:
                    below = U[t, y - 1, x + 1, mid, :]
                if y == NY - 1:
                    above = jnp.where(has_hi, H[t, 1, x], 0.0)
                else:
                    above = U[t, y + 1, x + 1, mid, :]
                left, right = U[t, y, x, mid, :], U[t, y, x + 2, mid, :]
                down = U[t, y, x + 1, pl.ds(ZP - 1, NZ), :]
                up = U[t, y, x + 1, pl.ds(ZP + 1, NZ), :]
                total = ((below + above) + (left + right)) + (down + up)
                flow = (
                    V[0, y, x] * (above - below)
                    + V[1, y, x] * (right - left)
                    + V[2, y, x] * (up - down)
                )
                spread = total - 6.0 * here
                new = (here - flow) + 0.05 * spread

                @pl.when(t + 1 < STEPS)
                def _():
                    U[jnp.minimum(t + 1, STEPS - 1), y, x + 1, mid, :] = new

                @pl.when(t + 1 == STEPS)
                def _():
                    out[y, x] = new

            return 0

        lax.fori_loop(0, XC, column, 0)

    def sends(j):
        t, i = j // K, j % K
        k = chunk(i)

        @pl.when(t + 1 < STEPS)
        def _():
            send_y(False, t + 1, i, k)
            z_copy(False, t + 1, k).start()

            @pl.when((i == 0) & x_lo)
            def _():
                x_copy(False, t + 1, 0).start()

            @pl.when((i == 1) & x_hi)
            def _():
                x_copy(False, t + 1, 1).start()


    def relay(n, due):
        t, i = n // K, n % K

        @pl.when(due & edge & through(t, i))
        def _():
            k = chunk(i)
            slot = jnp.where(py == 0, 0, 1)
            y_landed(t, slot, k).wait_recv()
            relay_copy(t, k).start()

    def iteration(j, _):
        t, i = j // K, j % K
        k = chunk(i)

        relay(2 * j, j < K - AHEAD)
        relay(2 * j + 1, j < K - AHEAD)
        relay(j + K - AHEAD, (j >= K - AHEAD) & (j + K - AHEAD < STEPS * K))

        @pl.when(t == 0)
        def _():
            @pl.when(i + PRE + 2 < K)
            def _():
                load_u(chunk(jnp.minimum(i + PRE + 2, K - 1))).start()

            @pl.when(i + PRE < K)
            def _():
                for f in range(3):
                    load_v(f, chunk(jnp.minimum(i + PRE, K - 1))).start()

            @pl.when(i == 0)
            def _():
                load_u(chunk(0)).wait()
                load_u(chunk(1)).wait()

            @pl.when(i + 2 < K)
            def _():
                load_u(chunk(jnp.minimum(i + 2, K - 1))).wait()

            for f in range(3):
                load_v(f, k).wait()

        @pl.when((i == 0) & x_lo)
        def _():
            x_landed(t, 0).wait_recv()

        @pl.when((i == 1) & x_hi)
        def _():
            x_landed(t, 1).wait_recv()

        z_copy(False, t, k).wait_recv()

        @pl.when(has_lo)
        def _():
            y_landed(t, 0, k).wait_recv()

        @pl.when(has_hi)
        def _():
            y_landed(t, 1, k).wait_recv()

        compute(t, k, (0, NY - 1))
        compute(t, k, range(1, NY - 1))
        sends(j)
        return 0

    def x_landed(t, side):
        column = (0, NX + 1)[side]
        return pltpu.make_async_remote_copy(
            src_ref=U.at[t, :, column, pl.ds(ZP, NZ)],
            dst_ref=U.at[t, :, column, pl.ds(ZP, NZ)],
            send_sem=x_send.at[t, side],
            recv_sem=x_recv.at[t, side],
            device_id={"px": jnp.where(px == 0, 1, 0)},
            device_id_type=MESH,
        )

    lax.fori_loop(0, STEPS * K, iteration, 0)

    def finish(j, _):
        t, i = j // K, j % K
        k = chunk(i)

        @pl.when(has_lo | (edge & through(t, i)))
        def _():
            y_landed(t, 0, k).wait_send()

        @pl.when(has_hi | (edge & through(t, i)))
        def _():
            y_landed(t, 1, k).wait_send()

        z_copy(False, t, k).wait_send()
        return 0

    lax.fori_loop(0, STEPS * K, finish, 0)
    for t in range(STEPS):
        for side, there in ((0, x_lo), (1, x_hi)):

            @pl.when(there)
            def _():
                x_landed(t, side).wait_send()


def body(u, vn, ve, vu):
    DMA = pltpu.SemaphoreType.DMA
    held = pl.pallas_call(
        kernel,
        out_shape=pltpu.VMEM(u.shape, u.dtype),
        in_specs=[pl.BlockSpec(memory_space=pl.ANY)] * 4,
        out_specs=pl.BlockSpec(memory_space=pltpu.VMEM),
        scratch_shapes=[
            pltpu.VMEM((STEPS, NY, NX + 2, NZ + 2 * ZP, NS), jnp.float32),
            pltpu.VMEM((3, NY, NX, NZ, NS), jnp.float32),
            pltpu.VMEM((STEPS, 2, NX, NZ, NS), jnp.float32),
            DMA((K,)),
            DMA((3, K)),
            DMA((K,)),
            DMA((STEPS, 2, K)),
            DMA((STEPS, 2, K)),
            DMA((STEPS, 2)),
            DMA((STEPS, 2)),
            DMA((STEPS, K)),
            DMA((STEPS, K)),
        ],
        compiler_params=pltpu.CompilerParams(
            collective_id=0, has_side_effects=True, vmem_limit_bytes=52 * 2**20
        ),
        name="march",
    )(u, vn, ve, vu)
    return held


def solution(mesh):
    spec = P(("site", "py"), "px", "pz", None)
    return jax.shard_map(
        body, mesh=mesh, in_specs=(spec,) * 4, out_specs=spec, check_vma=False
    )
```

```python
import functools

import jax
import jax.numpy as jnp
from jax import lax
from jax.experimental import pallas as pl
from jax.experimental.pallas import tpu as pltpu
from jax.sharding import PartitionSpec as P

MESH = pl.DeviceIdType.MESH
STEPS = 4
NY, NX, NZ, NS = 4, 64, 32, 128
K = 8
XC = NX // K
AHEAD = 2
PRE = 2
DIRECT = 0
DET0 = 1
DET1 = 1
DJ = 2
DMAX = max(DET0, DET1, 1)
ZP = 8


def kernel(u, vn, ve, vu, out, U, V, H, D, *sems):
    (u_sem, v_sem, h_send, h_recv, x_send, x_recv, z_send, z_recv, d_send, d_recv) = sems
    py, px, pz = lax.axis_index("py"), lax.axis_index("px"), lax.axis_index("pz")
    has_lo, has_hi = py > 0, py < 7
    x_lo, x_hi = px > 0, px < 3
    relayed = pz == 1
    edge = (py == 0) | (py == 7)
    middle = (py == 3) | (py == 4)

    def chunk(i):
        half = i // 2
        return half + (i % 2) * (K - 1 - 2 * half)

    def cols(k):
        return pl.ds(k * XC, XC)

    def inner(k):
        return pl.ds(1 + k * XC, XC)

    def load_u(k):
        return pltpu.make_async_copy(
            u.at[:, cols(k)], U.at[0, :, inner(k), pl.ds(ZP, NZ)], u_sem.at[k]
        )

    def load_v(f, k):
        return pltpu.make_async_copy(
            (vn, ve, vu)[f].at[:, cols(k)], V.at[f, :, cols(k)], v_sem.at[f, k]
        )

    def y_source(first, t, side, k):
        plane = (0, NY - 1)[side]
        if first:
            return u.at[plane, cols(k)]
        return U.at[t, plane, inner(k), pl.ds(ZP, NZ)]

    def y_copy(first, t, side, k, target, slot):
        return pltpu.make_async_remote_copy(
            src_ref=y_source(first, t, side, k),
            dst_ref=H.at[t, slot, cols(k)],
            send_sem=h_send.at[t, side, k],
            recv_sem=h_recv.at[t, slot, k],
            device_id={"py": target},
            device_id_type=MESH,
        )

    def through(t, i):
        late = (t == STEPS - 1) & (i >= K - DIRECT)
        return relayed & jnp.logical_not(late) & jnp.logical_not(detoured(t, i))

    def detoured(t, i):
        return (t == 0) & (i >= K - jnp.where(pz == 0, DET0, DET1))


    def y_route(t, i, side):
        if side == 0:
            return jnp.where((py == 4) & through(t, i), 7, jnp.maximum(py - 1, 0)), 1
        return jnp.where((py == 3) & through(t, i), 0, jnp.minimum(py + 1, 7)), 0

    def detour_copy(n):
        k = chunk(K - 1 - n)
        up = py == 3
        return pltpu.make_async_remote_copy(
            src_ref=u.at[jnp.where(up, NY - 1, 0), cols(k)],
            dst_ref=D.at[n],
            send_sem=h_send.at[0, jnp.where(up, 1, 0), k],
            recv_sem=d_recv.at[n],
            device_id={"py": jnp.where(up, 2, 5)},
            device_id_type=MESH,
        )

    def pass_copy(n):
        k = chunk(K - 1 - n)
        slot = jnp.where(py == 2, 0, 1)
        return pltpu.make_async_remote_copy(
            src_ref=D.at[n],
            dst_ref=H.at[0, slot, cols(k)],
            send_sem=d_send.at[n],
            recv_sem=h_recv.at[0, slot, k],
            device_id={"py": jnp.where(py == 2, 4, 3)},
            device_id_type=MESH,
        )

    def detour_landed(n):
        return pltpu.make_async_remote_copy(
            src_ref=D.at[n],
            dst_ref=D.at[n],
            send_sem=d_send.at[n],
            recv_sem=d_recv.at[n],
            device_id={"py": jnp.where(py == 2, 4, 3)},
            device_id_type=MESH,
        )

    beside = (py == 2) | (py == 5)
    detours = jnp.where(pz == 0, DET0, DET1)

    def send_y(first, t, i, k):
        skip = detoured(t, i) & first

        @pl.when(has_lo & ~(skip & (py == 4)))
        def _():
            y_copy(first, t, 0, k, *y_route(t, i, 0)).start()

        @pl.when(has_hi & ~(skip & (py == 3)))
        def _():
            y_copy(first, t, 1, k, *y_route(t, i, 1)).start()

    def relay_copy(t, k):
        slot = jnp.where(py == 0, 0, 1)
        return pltpu.make_async_remote_copy(
            src_ref=H.at[t, slot, cols(k)],
            dst_ref=H.at[t, slot, cols(k)],
            send_sem=h_send.at[t, slot, k],
            recv_sem=h_recv.at[t, slot, k],
            device_id={"py": jnp.where(py == 0, 4, 3)},
            device_id_type=MESH,
        )

    def y_landed(t, slot, k):
        return pltpu.make_async_remote_copy(
            src_ref=H.at[t, slot, cols(k)],
            dst_ref=H.at[t, slot, cols(k)],
            send_sem=h_send.at[t, slot, k],
            recv_sem=h_recv.at[t, slot, k],
            device_id={"py": jnp.where(py == 0, 1, 0)},
            device_id_type=MESH,
        )

    def x_copy(first, t, side):
        src, dst = ((0, NX + 1), (NX - 1, 0))[side]
        source = u.at[:, src] if first else U.at[t, :, 1 + src, pl.ds(ZP, NZ)]
        return pltpu.make_async_remote_copy(
            src_ref=source,
            dst_ref=U.at[t, :, dst, pl.ds(ZP, NZ)],
            send_sem=x_send.at[t, side],
            recv_sem=x_recv.at[t, 1 - side],
            device_id={"px": (jnp.maximum(px - 1, 0), jnp.minimum(px + 1, 3))[side]},
            device_id_type=MESH,
        )

    def z_copy(first, t, k):
        start = pl.multiple_of((1 - pz) * (NZ - ZP), ZP)
        if first:
            source = u.at[:, cols(k), pl.ds(start, ZP)]
        else:
            source = U.at[t, :, inner(k), pl.ds(pl.multiple_of(start + ZP, ZP), ZP)]
        land = pl.multiple_of(pz * (NZ + ZP), ZP)
        return pltpu.make_async_remote_copy(
            src_ref=source,
            dst_ref=U.at[t, :, inner(k), pl.ds(land, ZP)],
            send_sem=z_send.at[t, k],
            recv_sem=z_recv.at[t, k],
            device_id={"pz": 1 - pz},
            device_id_type=MESH,
        )

    barrier = pltpu.get_barrier_semaphore()

    def greet(cond, **where):
        @pl.when(cond)
        def _():
            pl.semaphore_signal(barrier, inc=1, device_id=where, device_id_type=MESH)

    meets = jnp.logical_not(relayed) | (DIRECT > 0)
    low = has_lo & ((py != 4) | meets)
    high = has_hi & ((py != 3) | meets)
    greet(low, py=jnp.maximum(py - 1, 0))
    greet(high, py=jnp.minimum(py + 1, 7))
    greet(x_lo, px=jnp.maximum(px - 1, 0))
    greet(x_hi, px=jnp.minimum(px + 1, 3))
    greet(pz >= 0, pz=1 - pz)
    ring = relayed & (edge | middle)
    source = jnp.where(py == 0, 3, jnp.where(py == 4, 0, jnp.where(py == 7, 4, 7)))
    greet(ring, py=source)
    greet(middle & (detours > 0), py=jnp.where(py == 4, 2, 5))
    one = lambda c: c.astype(jnp.int32)
    peers = one(low) + one(high) + one(x_lo) + one(x_hi) + 1 + one(ring)
    peers = peers + one(beside & (detours > 0))
    pl.semaphore_wait(barrier, peers)

    @pl.when(x_lo)
    def _():
        x_copy(True, 0, 0).start()

    @pl.when(x_hi)
    def _():
        x_copy(True, 0, 1).start()

    for n in range(DMAX):

        @pl.when(middle & (n < detours))
        def _():
            detour_copy(n).start()

    def first_sends(i, _):
        k = chunk(i)
        send_y(True, 0, i, k)
        z_copy(True, 0, k).start()
        return 0

    lax.fori_loop(0, K, first_sends, 0)

    for i in range(min(PRE + 2, K)):
        load_u(chunk(i)).start()
    for i in range(min(PRE, K)):
        for f in range(3):
            load_v(f, chunk(i)).start()

    zero_slab = pl.multiple_of(pz * (NZ + ZP), ZP)

    def clear_z(n, _):
        t, y = n // NY, n % NY
        U[t, y, :, pl.ds(zero_slab, ZP), :] = jnp.zeros((NX + 2, ZP, NS), jnp.float32)
        return 0

    lax.fori_loop(0, STEPS * NY, clear_z, 0)

    def clear_x(cond, column):
        @pl.when(cond)
        def _():
            for t in range(STEPS):
                U[t, :, column, pl.ds(ZP, NZ), :] = jnp.zeros((NY, NZ, NS), jnp.float32)

    clear_x(jnp.logical_not(x_lo), 0)
    clear_x(jnp.logical_not(x_hi), NX + 1)

    def compute(t, k, planes, last):
        def column(n, _):
            x = k * XC + n
            mid = pl.ds(ZP, NZ)
            for y in planes:
                here = U[t, y, x + 1, mid, :]
                if y == 0:
                    below = jnp.where(has_lo, H[t, 0, x], 0.0)
                else:
                    below = U[t, y - 1, x + 1, mid, :]
                if y == NY - 1:
                    above = jnp.where(has_hi, H[t, 1, x], 0.0)
                else:
                    above = U[t, y + 1, x + 1, mid, :]
                left, right = U[t, y, x, mid, :], U[t, y, x + 2, mid, :]
                down = U[t, y, x + 1, pl.ds(ZP - 1, NZ), :]
                up = U[t, y, x + 1, pl.ds(ZP + 1, NZ), :]
                total = ((below + above) + (left + right)) + (down + up)
                flow = (
                    V[0, y, x] * (above - below)
                    + V[1, y, x] * (right - left)
                    + V[2, y, x] * (up - down)
                )
                spread = total - 6.0 * here
                new = (here - flow) + 0.05 * spread
                if last:
                    out[y, x] = new
                else:
                    U[t + 1, y, x + 1, mid, :] = new
            return 0

        lax.fori_loop(0, XC, column, 0, unroll=2)

    def sends(j):
        t, i = j // K, j % K
        k = chunk(i)
        send_y(False, t + 1, i, k)
        z_copy(False, t + 1, k).start()

        @pl.when((i == 0) & x_lo)
        def _():
            x_copy(False, t + 1, 0).start()

        @pl.when((i == 1) & x_hi)
        def _():
            x_copy(False, t + 1, 1).start()

    def relay(n, due):
        t, i = n // K, n % K

        @pl.when(due & edge & through(t, i))
        def _():
            k = chunk(i)
            slot = jnp.where(py == 0, 0, 1)
            y_landed(t, slot, k).wait_recv()
            relay_copy(t, k).start()

    def iteration(j, _):
        t, i = j // K, j % K
        k = chunk(i)

        for n in range(DMAX):

            @pl.when(beside & (n < detours) & (j == DJ + DMAX - 1 - n))
            def _():
                detour_landed(n).wait_recv()
                pass_copy(n).start()

        relay(2 * j, j < K - AHEAD)
        relay(2 * j + 1, j < K - AHEAD)
        relay(j + K - AHEAD, (j >= K - AHEAD) & (j + K - AHEAD < STEPS * K))

        @pl.when(t == 0)
        def _():
            @pl.when(i + PRE + 2 < K)
            def _():
                load_u(chunk(jnp.minimum(i + PRE + 2, K - 1))).start()

            @pl.when(i + PRE < K)
            def _():
                for f in range(3):
                    load_v(f, chunk(jnp.minimum(i + PRE, K - 1))).start()

            @pl.when(i == 0)
            def _():
                load_u(chunk(0)).wait()
                load_u(chunk(1)).wait()

            @pl.when(i + 2 < K)
            def _():
                load_u(chunk(jnp.minimum(i + 2, K - 1))).wait()

            for f in range(3):
                load_v(f, k).wait()

        @pl.when((i == 0) & x_lo)
        def _():
            x_landed(t, 0).wait_recv()

        @pl.when((i == 1) & x_hi)
        def _():
            x_landed(t, 1).wait_recv()

        z_copy(False, t, k).wait_recv()

        @pl.when(t == STEPS - 1)
        def _():
            compute(t, k, range(1, NY - 1), True)

        @pl.when(has_lo)
        def _():
            y_landed(t, 0, k).wait_recv()

        @pl.when(has_hi)
        def _():
            y_landed(t, 1, k).wait_recv()

        @pl.when(t < STEPS - 1)
        def _():
            compute(t, k, (0, NY - 1), False)
            compute(t, k, range(1, NY - 1), False)
            sends(j)

        @pl.when(t == STEPS - 1)
        def _():
            compute(t, k, (0, NY - 1), True)

        return 0

    def x_landed(t, side):
        column = (0, NX + 1)[side]
        return pltpu.make_async_remote_copy(
            src_ref=U.at[t, :, column, pl.ds(ZP, NZ)],
            dst_ref=U.at[t, :, column, pl.ds(ZP, NZ)],
            send_sem=x_send.at[t, side],
            recv_sem=x_recv.at[t, side],
            device_id={"px": jnp.where(px == 0, 1, 0)},
            device_id_type=MESH,
        )

    lax.fori_loop(0, STEPS * K, iteration, 0)

    def finish(j, _):
        t, i = j // K, j % K
        k = chunk(i)

        @pl.when(has_lo | (edge & through(t, i)))
        def _():
            y_landed(t, 0, k).wait_send()

        @pl.when(has_hi | (edge & through(t, i)))
        def _():
            y_landed(t, 1, k).wait_send()

        z_copy(False, t, k).wait_send()
        return 0

    lax.fori_loop(0, STEPS * K, finish, 0)
    for n in range(DMAX):

        @pl.when(beside & (n < detours))
        def _():
            pass_copy(n).wait_send()

    for t in range(STEPS):
        for side, there in ((0, x_lo), (1, x_hi)):

            @pl.when(there)
            def _():
                x_landed(t, side).wait_send()


def body(u, vn, ve, vu):
    DMA = pltpu.SemaphoreType.DMA
    held = pl.pallas_call(
        kernel,
        out_shape=pltpu.VMEM(u.shape, u.dtype),
        in_specs=[pl.BlockSpec(memory_space=pl.ANY)] * 4,
        out_specs=pl.BlockSpec(memory_space=pltpu.VMEM),
        scratch_shapes=[
            pltpu.VMEM((STEPS, NY, NX + 2, NZ + 2 * ZP, NS), jnp.float32),
            pltpu.VMEM((3, NY, NX, NZ, NS), jnp.float32),
            pltpu.VMEM((STEPS, 2, NX, NZ, NS), jnp.float32),
            pltpu.VMEM((DMAX, XC, NZ, NS), jnp.float32),
            DMA((K,)),
            DMA((3, K)),
            DMA((STEPS, 2, K)),
            DMA((STEPS, 2, K)),
            DMA((STEPS, 2)),
            DMA((STEPS, 2)),
            DMA((STEPS, K)),
            DMA((STEPS, K)),
            DMA((DMAX,)),
            DMA((DMAX,)),
        ],
        compiler_params=pltpu.CompilerParams(
            collective_id=0, has_side_effects=True, vmem_limit_bytes=52 * 2**20
        ),
        name="march",
    )(u, vn, ve, vu)
    return held


def solution(mesh):
    spec = P(("site", "py"), "px", "pz", None)
    return jax.shard_map(
        body, mesh=mesh, in_specs=(spec,) * 4, out_specs=spec, check_vma=False
    )
```

```python
import functools

import jax
import jax.numpy as jnp
from jax import lax
from jax.experimental import pallas as pl
from jax.experimental.pallas import tpu as pltpu
from jax.sharding import PartitionSpec as P

MESH = pl.DeviceIdType.MESH
STEPS = 4
NY, NX, NZ, NS = 4, 64, 32, 128
K = 8
XC = NX // K
AHEAD = 2
PRE = 2
DA = 0
DB = 2
DET0 = 1
DET1 = 1
DJ = 2
DMAX = max(DET0, DET1, 1)
ZP = 8


def kernel(u, vn, ve, vu, out, U, V, H, D, *sems):
    (u_sem, v_sem, h_send, h_recv, x_send, x_recv, z_send, z_recv, d_send, d_recv) = sems
    py, px, pz = lax.axis_index("py"), lax.axis_index("px"), lax.axis_index("pz")
    has_lo, has_hi = py > 0, py < 7
    x_lo, x_hi = px > 0, px < 3
    relayed = pz == 1
    site = lax.axis_index("site")
    outer = (site == 0) | (site == 3)
    by_a, by_b = (
        (site >= 0) & (w > 0) & ((w != 2) | outer) & ((w != 3) | ~outer) for w in (DA, DB)
    )
    edge = (py == 0) | (py == 7)
    middle = (py == 3) | (py == 4)

    def chunk(i):
        half = i // 2
        return half + (i % 2) * (K - 1 - 2 * half)

    def cols(k):
        return pl.ds(k * XC, XC)

    def inner(k):
        return pl.ds(1 + k * XC, XC)

    def load_u(k):
        return pltpu.make_async_copy(
            u.at[:, cols(k)], U.at[0, :, inner(k), pl.ds(ZP, NZ)], u_sem.at[k]
        )

    def load_v(f, k):
        return pltpu.make_async_copy(
            (vn, ve, vu)[f].at[:, cols(k)], V.at[f, :, cols(k)], v_sem.at[f, k]
        )

    def y_source(first, t, side, k):
        plane = (0, NY - 1)[side]
        if first:
            return u.at[plane, cols(k)]
        return U.at[t, plane, inner(k), pl.ds(ZP, NZ)]

    def y_copy(first, t, side, k, target, slot):
        return pltpu.make_async_remote_copy(
            src_ref=y_source(first, t, side, k),
            dst_ref=H.at[t, slot, cols(k)],
            send_sem=h_send.at[t, side, k],
            recv_sem=h_recv.at[t, slot, k],
            device_id={"py": target},
            device_id_type=MESH,
        )

    def through(t, i):
        late = (t == STEPS - 1) & (i == K - 1) & jnp.where((py == 3) | (py == 0), by_a, by_b)
        return relayed & jnp.logical_not(late) & jnp.logical_not(detoured(t, i))

    def detoured(t, i):
        return (t == 0) & (i >= K - jnp.where(pz == 0, DET0, DET1))


    def y_route(t, i, side):
        if side == 0:
            return jnp.where((py == 4) & through(t, i), 7, jnp.maximum(py - 1, 0)), 1
        return jnp.where((py == 3) & through(t, i), 0, jnp.minimum(py + 1, 7)), 0

    def detour_copy(n):
        k = chunk(K - 1 - n)
        up = py == 3
        return pltpu.make_async_remote_copy(
            src_ref=u.at[jnp.where(up, NY - 1, 0), cols(k)],
            dst_ref=D.at[n],
            send_sem=h_send.at[0, jnp.where(up, 1, 0), k],
            recv_sem=d_recv.at[n],
            device_id={"py": jnp.where(up, 2, 5)},
            device_id_type=MESH,
        )

    def pass_copy(n):
        k = chunk(K - 1 - n)
        slot = jnp.where(py == 2, 0, 1)
        return pltpu.make_async_remote_copy(
            src_ref=D.at[n],
            dst_ref=H.at[0, slot, cols(k)],
            send_sem=d_send.at[n],
            recv_sem=h_recv.at[0, slot, k],
            device_id={"py": jnp.where(py == 2, 4, 3)},
            device_id_type=MESH,
        )

    def detour_landed(n):
        return pltpu.make_async_remote_copy(
            src_ref=D.at[n],
            dst_ref=D.at[n],
            send_sem=d_send.at[n],
            recv_sem=d_recv.at[n],
            device_id={"py": jnp.where(py == 2, 4, 3)},
            device_id_type=MESH,
        )

    beside = (py == 2) | (py == 5)
    detours = jnp.where(pz == 0, DET0, DET1)

    def send_y(first, t, i, k):
        skip = detoured(t, i) & first

        @pl.when(has_lo & ~(skip & (py == 4)))
        def _():
            y_copy(first, t, 0, k, *y_route(t, i, 0)).start()

        @pl.when(has_hi & ~(skip & (py == 3)))
        def _():
            y_copy(first, t, 1, k, *y_route(t, i, 1)).start()

    def relay_copy(t, k):
        slot = jnp.where(py == 0, 0, 1)
        return pltpu.make_async_remote_copy(
            src_ref=H.at[t, slot, cols(k)],
            dst_ref=H.at[t, slot, cols(k)],
            send_sem=h_send.at[t, slot, k],
            recv_sem=h_recv.at[t, slot, k],
            device_id={"py": jnp.where(py == 0, 4, 3)},
            device_id_type=MESH,
        )

    def y_landed(t, slot, k):
        return pltpu.make_async_remote_copy(
            src_ref=H.at[t, slot, cols(k)],
            dst_ref=H.at[t, slot, cols(k)],
            send_sem=h_send.at[t, slot, k],
            recv_sem=h_recv.at[t, slot, k],
            device_id={"py": jnp.where(py == 0, 1, 0)},
            device_id_type=MESH,
        )

    def x_copy(first, t, side):
        src, dst = ((0, NX + 1), (NX - 1, 0))[side]
        source = u.at[:, src] if first else U.at[t, :, 1 + src, pl.ds(ZP, NZ)]
        return pltpu.make_async_remote_copy(
            src_ref=source,
            dst_ref=U.at[t, :, dst, pl.ds(ZP, NZ)],
            send_sem=x_send.at[t, side],
            recv_sem=x_recv.at[t, 1 - side],
            device_id={"px": (jnp.maximum(px - 1, 0), jnp.minimum(px + 1, 3))[side]},
            device_id_type=MESH,
        )

    def z_copy(first, t, k):
        start = pl.multiple_of((1 - pz) * (NZ - ZP), ZP)
        if first:
            source = u.at[:, cols(k), pl.ds(start, ZP)]
        else:
            source = U.at[t, :, inner(k), pl.ds(pl.multiple_of(start + ZP, ZP), ZP)]
        land = pl.multiple_of(pz * (NZ + ZP), ZP)
        return pltpu.make_async_remote_copy(
            src_ref=source,
            dst_ref=U.at[t, :, inner(k), pl.ds(land, ZP)],
            send_sem=z_send.at[t, k],
            recv_sem=z_recv.at[t, k],
            device_id={"pz": 1 - pz},
            device_id_type=MESH,
        )

    barrier = pltpu.get_barrier_semaphore()

    def greet(cond, **where):
        @pl.when(cond)
        def _():
            pl.semaphore_signal(barrier, inc=1, device_id=where, device_id_type=MESH)

    plain = jnp.logical_not(relayed)
    greet(has_lo & ((py != 4) | plain | by_a), py=jnp.maximum(py - 1, 0))
    greet(has_hi & ((py != 3) | plain | by_b), py=jnp.minimum(py + 1, 7))
    low = has_lo & ((py != 4) | plain | by_b)
    high = has_hi & ((py != 3) | plain | by_a)
    greet(x_lo, px=jnp.maximum(px - 1, 0))
    greet(x_hi, px=jnp.minimum(px + 1, 3))
    greet(pz >= 0, pz=1 - pz)
    ring = relayed & (edge | middle)
    source = jnp.where(py == 0, 3, jnp.where(py == 4, 0, jnp.where(py == 7, 4, 7)))
    greet(ring, py=source)
    greet(middle & (detours > 0), py=jnp.where(py == 4, 2, 5))
    one = lambda c: c.astype(jnp.int32)
    peers = one(low) + one(high) + one(x_lo) + one(x_hi) + 1 + one(ring)
    peers = peers + one(beside & (detours > 0))
    pl.semaphore_wait(barrier, peers)

    @pl.when(x_lo)
    def _():
        x_copy(True, 0, 0).start()

    @pl.when(x_hi)
    def _():
        x_copy(True, 0, 1).start()

    for n in range(DMAX):

        @pl.when(middle & (n < detours))
        def _():
            detour_copy(n).start()

    def first_sends(i, _):
        k = chunk(i)
        send_y(True, 0, i, k)
        z_copy(True, 0, k).start()
        return 0

    lax.fori_loop(0, K, first_sends, 0)

    for i in range(min(PRE + 2, K)):
        load_u(chunk(i)).start()
    for i in range(min(PRE, K)):
        for f in range(3):
            load_v(f, chunk(i)).start()

    zero_slab = pl.multiple_of(pz * (NZ + ZP), ZP)

    def clear_z(n, _):
        t, y = n // NY, n % NY
        U[t, y, :, pl.ds(zero_slab, ZP), :] = jnp.zeros((NX + 2, ZP, NS), jnp.float32)
        return 0

    lax.fori_loop(0, STEPS * NY, clear_z, 0)

    def clear_x(cond, column):
        @pl.when(cond)
        def _():
            for t in range(STEPS):
                U[t, :, column, pl.ds(ZP, NZ), :] = jnp.zeros((NY, NZ, NS), jnp.float32)

    clear_x(jnp.logical_not(x_lo), 0)
    clear_x(jnp.logical_not(x_hi), NX + 1)

    def compute(t, k, planes, last):
        def column(n, _):
            x = k * XC + n
            mid = pl.ds(ZP, NZ)
            for y in planes:
                here = U[t, y, x + 1, mid, :]
                if y == 0:
                    below = jnp.where(has_lo, H[t, 0, x], 0.0)
                else:
                    below = U[t, y - 1, x + 1, mid, :]
                if y == NY - 1:
                    above = jnp.where(has_hi, H[t, 1, x], 0.0)
                else:
                    above = U[t, y + 1, x + 1, mid, :]
                left, right = U[t, y, x, mid, :], U[t, y, x + 2, mid, :]
                down = U[t, y, x + 1, pl.ds(ZP - 1, NZ), :]
                up = U[t, y, x + 1, pl.ds(ZP + 1, NZ), :]
                total = ((below + above) + (left + right)) + (down + up)
                flow = (
                    V[0, y, x] * (above - below)
                    + V[1, y, x] * (right - left)
                    + V[2, y, x] * (up - down)
                )
                spread = total - 6.0 * here
                new = (here - flow) + 0.05 * spread
                if last:
                    out[y, x] = new
                else:
                    U[t + 1, y, x + 1, mid, :] = new
            return 0

        lax.fori_loop(0, XC, column, 0, unroll=2)

    def sends(j):
        t, i = j // K, j % K
        k = chunk(i)
        send_y(False, t + 1, i, k)
        z_copy(False, t + 1, k).start()

        @pl.when((i == 0) & x_lo)
        def _():
            x_copy(False, t + 1, 0).start()

        @pl.when((i == 1) & x_hi)
        def _():
            x_copy(False, t + 1, 1).start()

    def relay(n, due):
        t, i = n // K, n % K

        @pl.when(due & edge & through(t, i))
        def _():
            k = chunk(i)
            slot = jnp.where(py == 0, 0, 1)
            y_landed(t, slot, k).wait_recv()
            relay_copy(t, k).start()

    def iteration(j, _):
        t, i = j // K, j % K
        k = chunk(i)

        for n in range(DMAX):

            @pl.when(beside & (n < detours) & (j == DJ + DMAX - 1 - n))
            def _():
                detour_landed(n).wait_recv()
                pass_copy(n).start()

        relay(2 * j, j < K - AHEAD)
        relay(2 * j + 1, j < K - AHEAD)
        relay(j + K - AHEAD, (j >= K - AHEAD) & (j + K - AHEAD < STEPS * K))

        @pl.when(t == 0)
        def _():
            @pl.when(i + PRE + 2 < K)
            def _():
                load_u(chunk(jnp.minimum(i + PRE + 2, K - 1))).start()

            @pl.when(i + PRE < K)
            def _():
                for f in range(3):
                    load_v(f, chunk(jnp.minimum(i + PRE, K - 1))).start()

            @pl.when(i == 0)
            def _():
                load_u(chunk(0)).wait()
                load_u(chunk(1)).wait()

            @pl.when(i + 2 < K)
            def _():
                load_u(chunk(jnp.minimum(i + 2, K - 1))).wait()

            for f in range(3):
                load_v(f, k).wait()

        @pl.when((i == 0) & x_lo)
        def _():
            x_landed(t, 0).wait_recv()

        @pl.when((i == 1) & x_hi)
        def _():
            x_landed(t, 1).wait_recv()

        z_copy(False, t, k).wait_recv()

        @pl.when(t == STEPS - 1)
        def _():
            compute(t, k, range(1, NY - 1), True)

        @pl.when(has_lo)
        def _():
            y_landed(t, 0, k).wait_recv()

        @pl.when(has_hi)
        def _():
            y_landed(t, 1, k).wait_recv()

        @pl.when(t < STEPS - 1)
        def _():
            compute(t, k, (0, NY - 1), False)
            compute(t, k, range(1, NY - 1), False)
            sends(j)

        @pl.when(t == STEPS - 1)
        def _():
            compute(t, k, (0, NY - 1), True)

        return 0

    def x_landed(t, side):
        column = (0, NX + 1)[side]
        return pltpu.make_async_remote_copy(
            src_ref=U.at[t, :, column, pl.ds(ZP, NZ)],
            dst_ref=U.at[t, :, column, pl.ds(ZP, NZ)],
            send_sem=x_send.at[t, side],
            recv_sem=x_recv.at[t, side],
            device_id={"px": jnp.where(px == 0, 1, 0)},
            device_id_type=MESH,
        )

    lax.fori_loop(0, STEPS * K, iteration, 0)

    def finish(j, _):
        t, i = j // K, j % K
        k = chunk(i)

        @pl.when(has_lo | (edge & through(t, i)))
        def _():
            y_landed(t, 0, k).wait_send()

        @pl.when(has_hi | (edge & through(t, i)))
        def _():
            y_landed(t, 1, k).wait_send()

        z_copy(False, t, k).wait_send()
        return 0

    lax.fori_loop(0, STEPS * K, finish, 0)
    for n in range(DMAX):

        @pl.when(beside & (n < detours))
        def _():
            pass_copy(n).wait_send()

    for t in range(STEPS):
        for side, there in ((0, x_lo), (1, x_hi)):

            @pl.when(there)
            def _():
                x_landed(t, side).wait_send()


def body(u, vn, ve, vu):
    DMA = pltpu.SemaphoreType.DMA
    held = pl.pallas_call(
        kernel,
        out_shape=pltpu.VMEM(u.shape, u.dtype),
        in_specs=[pl.BlockSpec(memory_space=pl.ANY)] * 4,
        out_specs=pl.BlockSpec(memory_space=pltpu.VMEM),
        scratch_shapes=[
            pltpu.VMEM((STEPS, NY, NX + 2, NZ + 2 * ZP, NS), jnp.float32),
            pltpu.VMEM((3, NY, NX, NZ, NS), jnp.float32),
            pltpu.VMEM((STEPS, 2, NX, NZ, NS), jnp.float32),
            pltpu.VMEM((DMAX, XC, NZ, NS), jnp.float32),
            DMA((K,)),
            DMA((3, K)),
            DMA((STEPS, 2, K)),
            DMA((STEPS, 2, K)),
            DMA((STEPS, 2)),
            DMA((STEPS, 2)),
            DMA((STEPS, K)),
            DMA((STEPS, K)),
            DMA((DMAX,)),
            DMA((DMAX,)),
        ],
        compiler_params=pltpu.CompilerParams(
            collective_id=0, has_side_effects=True, vmem_limit_bytes=52 * 2**20
        ),
        name="march",
    )(u, vn, ve, vu)
    return held


def solution(mesh):
    spec = P(("site", "py"), "px", "pz", None)
    return jax.shard_map(
        body, mesh=mesh, in_specs=(spec,) * 4, out_specs=spec, check_vma=False
    )
```
